32 devices in a mesh: gz: 4 (over z), gy: 4 (over x, core), gx: 2 (over y).
Axes of the slice: x: 2, y: 2, z: 4, core: 2. Of those that a mesh axis runs over, the one named last changes fastest.
Arguments:
- start: float32 [128, 64, 256], P('gz', 'gy', 'gx'), may hold values from -21 to 21
- measured: float32 [128, 8, 1024], P(('gz', 'gy', 'gx')), may hold values from -18 to 18
- tiles: bfloat16 [8192, 8, 512], P('gy', None, 'gx'), may hold values from -0.125 to 0.125
- tile_block: int32 [4, 2, 8], replicated, may hold values from 0 to 3
- angle_row: int32 [8], replicated, may hold values from 0 to 7, each once
Outputs:
- estimate: float32 [128, 64, 256], P('gz', 'gy', 'gx')
- dual_state: float32 [3, 128, 64, 256], P(None, 'gz', 'gy', 'gx')
The draws below stay inside these ranges and needn't reach their ends.
Inputs may be any that keep to these rules, and one draw needn't show every extreme that they name: `tile_block`: which of the 4 detector blocks of 256 columns each brick's tile covers at each angle. `angle_row`: every row of measured is named once.
All inputs are finite; a program needn't handle non-finite values.
Results may differ from the reference program's by a relative error of at most 0.0008.
Values may be sent and summed in bfloat16 or wider, within the bound.
A program may use at most 128 MiB of HBM per device.

```python
import jax
import jax.numpy as jnp
from jax import lax

CY = 16
CX = 128
ANG = 8
DW = 256
NBLK = 4
RADIUS = 8
ITERS = 2
V = 2048
DET = 1024
BRICKS_Y = 4
BRICKS_X = 2
NZ = 128
NY = 64
NX = 256
N_GY = 4
N_GX = 2


def draw_start(key, part):
    depth_at = jnp.arange(NZ, dtype=jnp.float32)[:, None, None] / NZ
    height_at = jnp.arange(NY, dtype=jnp.float32)[None, :, None] / NY
    breadth_at = jnp.arange(NX, dtype=jnp.float32)[None, None, :] / NX
    position = depth_at + height_at + breadth_at
    ramp = jnp.exp(jnp.log(3.0) * (position - 1.5))
    rough = jnp.clip(jax.random.normal(key, (NZ, NY, NX), jnp.float32), -4.0, 4.0)
    return ramp * rough


def plant(result, stream_key, low, high):
    shape = result.shape
    index_at = [jax.random.randint(jax.random.fold_in(stream_key, axis), (), 0, shape[axis]) for axis in range(len(shape))]
    result = result.at[tuple(index_at)].set(low)
    longest = shape.index(max(shape))
    index_at[longest] = (index_at[longest] + 1) % shape[longest]
    return result.at[tuple(index_at)].set(high)


def steps_of(stream_key, shape, split, low, top_value):
    def one(axis_at, blocks):
        heights = jax.random.uniform(jax.random.fold_in(jax.random.fold_in(stream_key, 6), axis_at), (blocks,), jnp.float32, low / len(split), top_value / len(split))
        return jnp.repeat(jnp.exp(heights), shape[axis_at] // blocks).reshape((-1,) + (1,) * (len(shape) - axis_at - 1))

    gain = one(*split[0])
    for cut in split[1:]:
        gain = gain * one(*cut)
    return gain


def centred(key, extent, width, reach, shards=(), kind=jnp.bfloat16):
    gain = steps_of(key, extent, shards, -0.22, 0.18) if shards else 1.0
    result = jax.random.normal(key, extent, jnp.float32) * width * gain
    return jnp.minimum(jnp.maximum(result, -reach), reach).astype(kind)


def setup_inputs(seed: int = 0) -> dict:
    key_of = jax.random.split(jax.random.key(seed), 6)
    start = draw_start(jax.random.fold_in(key_of[5], 71), 0)
    measured = centred(key_of[1], (NZ, ANG, DET), 3.0, 18.0, ((0, 32),), jnp.float32)
    tiles = centred(key_of[2], (BRICKS_Y * V, ANG, BRICKS_X * DW), V ** -0.5, 0.125, ((0, 4), (2, 2)))
    tile_block = plant(jax.random.randint(key_of[3], (BRICKS_Y, BRICKS_X, ANG), 0, NBLK), jax.random.fold_in(key_of[3], 1), 0, NBLK - 1).astype(jnp.int32)
    angle_row = jax.random.permutation(key_of[4], ANG).astype(jnp.int32)
    return dict(start=start, measured=measured, tiles=tiles, tile_block=tile_block, angle_row=angle_row)


blur_sigma = 2.5
step_size = 0.5
shrink_weight = 0.2
rho_start = 1.0
eps_norm = 1e-6


def blur_weights():
    offsets = jnp.arange(-RADIUS, RADIUS + 1).astype(jnp.float32)
    raw = jnp.exp(-offsets * offsets / (2.0 * blur_sigma * blur_sigma))
    return raw / jnp.sum(raw)


def blur_valid(padded, weights, axis, length):
    total = weights[0] * lax.slice_in_dim(padded, 0, length, axis=axis)
    for offset in range(1, 2 * RADIUS + 1):
        total = total + weights[offset] * lax.slice_in_dim(padded, offset, offset + length, axis=axis)
    return total


def blur_volume(field, weights):
    for axis in range(3):
        widths = [(0, 0), (0, 0), (0, 0)]
        widths[axis] = (RADIUS, RADIUS)
        field = blur_valid(jnp.pad(field, widths), weights, axis, field.shape[axis])
    return field


def select_blocks(spread, own_blocks):
    chosen = spread[:, :, 0, :]
    for block in range(1, NBLK):
        chosen = jnp.where((own_blocks == block)[None, :, None], spread[:, :, block, :], chosen)
    return chosen


def project(volume, tiles, tile_block):
    sino = jnp.zeros((NZ, ANG, NBLK, DW), jnp.float32)
    blocks = jnp.arange(NBLK, dtype=jnp.int32)
    for brow in range(N_GY):
        for bcol in range(N_GX):
            brick = volume[:, brow * CY:(brow + 1) * CY, bcol * CX:(bcol + 1) * CX].reshape(NZ, V)
            tile = tiles[brow * V:(brow + 1) * V, :, bcol * DW:(bcol + 1) * DW].reshape(V, ANG * DW)
            contrib = jnp.dot(brick, tile, preferred_element_type=jnp.float32).reshape(NZ, ANG, DW)
            onehot = (tile_block[brow, bcol][:, None] == blocks[None, :]).astype(jnp.float32)
            sino = sino + contrib[:, :, None, :] * onehot[None, :, :, None]
    return sino.reshape(NZ, ANG, NBLK * DW)


def backproject(misfit, tiles, tile_block):
    spread = misfit.reshape(NZ, ANG, NBLK, DW)
    slabs = []
    for brow in range(N_GY):
        pieces = []
        for bcol in range(N_GX):
            chosen = select_blocks(spread, tile_block[brow, bcol]).reshape(NZ, ANG * DW)
            tile = tiles[brow * V:(brow + 1) * V, :, bcol * DW:(bcol + 1) * DW].reshape(V, ANG * DW)
            back = lax.dot_general(chosen, tile, (((1,), (1,)), ((), ())), preferred_element_type=jnp.float32)
            pieces.append(back.reshape(NZ, CY, CX))
        slabs.append(jnp.concatenate(pieces, axis=2))
    return jnp.concatenate(slabs, axis=1)


def adjoint_one(values, axis):
    length = values.shape[axis]
    zero_slab = jnp.zeros_like(lax.slice_in_dim(values, 0, 1, axis=axis))
    before = jnp.concatenate([zero_slab, lax.slice_in_dim(values, 0, length - 1, axis=axis)], axis=axis)
    current = jnp.concatenate([lax.slice_in_dim(values, 0, length - 1, axis=axis), zero_slab], axis=axis)
    return before - current


def forward_terms(field):
    diffs = []
    smoothing = None
    for axis in range(3):
        zero_slab = jnp.zeros_like(lax.slice_in_dim(field, 0, 1, axis=axis))
        diff = jnp.concatenate([jnp.diff(field, axis=axis), zero_slab], axis=axis)
        term = adjoint_one(diff, axis)
        smoothing = term if smoothing is None else smoothing + term
        diffs.append(diff)
    return jnp.stack(diffs), smoothing


def adjoint_terms(stack):
    results = []
    for group in range(stack.shape[0] // 3):
        total = None
        for axis in range(3):
            term = adjoint_one(stack[group * 3 + axis], axis)
            total = term if total is None else total + term
        results.append(total)
    return results


def reference(start, measured, tiles, tile_block, angle_row):
    weights = blur_weights()
    observed = jnp.take(measured, angle_row, axis=1)
    cells = float(NZ * NY * NX)
    field = start
    jumps, smoothing = forward_terms(field)
    penalty = jnp.float32(rho_start)
    cutoff = shrink_weight / penalty
    shrunk = jumps - jnp.clip(jumps, -cutoff, cutoff)
    dual = jnp.zeros_like(jumps)
    back_shrunk = adjoint_terms(shrunk)[0]
    back_dual = jnp.zeros_like(field)
    for sweep in range(ITERS):
        blurred = blur_volume(field, weights).astype(jnp.bfloat16)
        sino = project(blurred, tiles, tile_block)
        misfit = (sino - observed).astype(jnp.bfloat16)
        data_grad = blur_volume(backproject(misfit, tiles, tile_block), weights)
        field = field - step_size * (data_grad + penalty * (smoothing + back_dual - back_shrunk))
        jumps, smoothing = forward_terms(field)
        total = jumps + dual
        shrunk_new = total - jnp.clip(total, -cutoff, cutoff)
        dual = total - shrunk_new
        if sweep + 1 < ITERS:
            back_dual, back_new = adjoint_terms(jnp.concatenate([dual, shrunk_new]))
        else:
            back_new = adjoint_terms(shrunk_new)[0]
        primal_sum = jnp.sum(jnp.square(jumps - shrunk_new))
        dual_sum = jnp.sum(jnp.square(back_new - back_shrunk))
        primal_res = primal_sum / (3.0 * cells)
        dual_res = penalty * penalty * dual_sum / cells
        factor = ((primal_res + eps_norm) / (dual_res + eps_norm)) ** 0.25
        penalty = penalty * factor
        cutoff = shrink_weight / penalty
        dual = dual / factor
        back_dual = back_dual / factor
        shrunk = shrunk_new
        back_shrunk = back_new
    return (field, dual)
```

```python
import functools
import math

import jax
import jax.numpy as jnp
from jax import lax
from jax.experimental import pallas as pl
from jax.experimental.pallas import tpu as pltpu
from jax.sharding import PartitionSpec as P

RADIUS = 8
ITERS = 2
NBLK = 4

blur_sigma = 2.5
step_size = 0.5
shrink_weight = 0.2
rho_start = 1.0
eps_norm = 1e-06

AXES = ("gz", "gy", "gx")
MESH = pl.DeviceIdType.MESH
HIGH = lax.Precision.HIGHEST
SPREAD = 2.0 * blur_sigma * blur_sigma
NORM = 1.0 / sum(math.exp(-k * k / SPREAD) for k in range(-RADIUS, RADIUS + 1))
TAPS = [NORM * math.exp(-k * k / SPREAD) for k in range(-RADIUS, RADIUS + 1)]
FACES = [(axis, side) for axis in AXES for side in (-1, 1)]
HALOS = [(dz, dy) for dz in (-1, 0, 1) for dy in (-1, 0, 1) if dz or dy]


def band(distance):
    near = jnp.abs(distance) <= RADIUS
    d = distance.astype(jnp.float32)
    return jnp.where(near, jnp.exp(-d * d / SPREAD) * NORM, 0.0)


def iota(shape, dim):
    return lax.broadcasted_iota(jnp.int32, shape, dim)


def dot(a, b, precision=None):
    return jnp.dot(a, b, preferred_element_type=jnp.float32, precision=precision)


def kernel(sizes, dims, start_ref, measured_ref, tiles_ref, table_ref, rows_ref, estimate_ref, dual_ref, *scratch):
    (raw, mats, ext, yb, flat, proj, send1, recv1, send2, arrived, misfit,
     hy_send, hz_send, hc_send, hy, hz, hc, x_send, x_recv, fy_send, fz_send, fx_send, fy, fz, fx,
     sum_send, sum_recv, field_ref, base_ref, back_ref, dual_s, dlow_s, send_sem, recv_sem, load_sem) = scratch
    CZ, CY, CX, ANG, DW, V, owned = dims
    bricks = sizes["gy"] * sizes["gx"]
    ngx = sizes["gx"]
    at = {axis: lax.axis_index(axis) for axis in AXES}
    me = at["gy"] * ngx + at["gx"]
    counter = [0]
    R = RADIUS
    cells = float(CZ * CY * CX * sizes["gz"] * bricks)

    def exists(steps):
        ok = None
        for axis, step in steps.items():
            if step == 0:
                continue
            test = at[axis] > 0 if step < 0 else at[axis] < sizes[axis] - 1
            ok = test if ok is None else jnp.logical_and(ok, test)
        return ok

    def remote(src, dst, target):
        slot = counter[0]
        counter[0] += 1
        return pltpu.make_async_remote_copy(
            src_ref=src, dst_ref=dst, send_sem=send_sem.at[slot], recv_sem=recv_sem.at[slot],
            device_id=target, device_id_type=MESH)

    def shift_send(src, dst_here, dst_there, steps):
        target = {axis: lax.rem(at[axis] + step + sizes[axis], sizes[axis]) for axis, step in steps.items() if step}
        copy = remote(src, dst_there, target)
        out_ok = exists(steps)
        in_ok = exists({axis: -step for axis, step in steps.items()})

        @pl.when(out_ok)
        def _():
            copy.start()

        @pl.when(jnp.logical_not(in_ok))
        def _():
            dst_here[...] = jnp.zeros(dst_here.shape, dst_here.dtype)

        def finish():
            @pl.when(out_ok)
            def _():
                copy.wait_send()

            @pl.when(in_ok)
            def _():
                copy.wait_recv()
        return finish

    chunks = 8
    per = V * ANG // chunks
    loads = [pltpu.make_async_copy(tiles_ref.at[pl.ds(i * per, per)], raw.at[pl.ds(i * per, per)], load_sem.at[i])
             for i in range(chunks)]
    for load in loads:
        load.start()
    group = 256 // ANG
    r, c = iota((256, 256), 0), iota((256, 256), 1)
    to_major = jnp.where((r // group == c % ANG) & (r % group == c // ANG), 1.0, 0.0).astype(jnp.bfloat16)

    def relayout():
        steps = per // 256
        for i in range(chunks):
            loads[i].wait()

            def one(n, carry):
                block = raw[pl.ds(pl.multiple_of(i * per + n * 256, 256), 256), :]
                moved = dot(to_major, block).astype(jnp.bfloat16)
                first = pl.multiple_of((i * steps + n) * group, group)
                for a in range(ANG):
                    mats[a, pl.ds(first, group), :] = moved[a * group:(a + 1) * group]
                return carry
            lax.fori_loop(0, steps, one, 0)

    def permute(block, transposed):
        n = CZ * ANG
        rr, cc = iota((n, n), 0), iota((n, n), 1)
        if transposed:
            m = (rr // ANG == cc % CZ) & (rr % ANG == cc // CZ)
        else:
            m = (rr // CZ == cc % ANG) & (rr % CZ == cc // ANG)
        return dot(jnp.where(m, 1.0, 0.0).astype(jnp.bfloat16), block)

    def halo_start(b, value):
        low = value.astype(jnp.bfloat16)
        hy_send[0] = low[CY - R:]
        hy_send[1] = low[:R]
        zl, zh = value[:, CZ - R:, :].astype(jnp.bfloat16), value[:, :R, :].astype(jnp.bfloat16)
        hz_send[0] = zl
        hz_send[1] = zh
        hc_send[0] = zl[CY - R:]
        hc_send[1] = zl[:R]
        hc_send[2] = zh[CY - R:]
        hc_send[3] = zh[:R]
        ends = []
        for side, step in ((0, 1), (1, -1)):
            ends.append(shift_send(hy_send.at[side], hy.at[b, side], hy.at[b, side], {"gy": step}))
            ends.append(shift_send(hz_send.at[side], hz.at[b, side], hz.at[b, side], {"gz": step}))
        for zs, zstep in ((0, 1), (1, -1)):
            for ys, ystep in ((0, 1), (1, -1)):
                s = zs * 2 + ys
                ends.append(shift_send(hc_send.at[s], hc.at[b, s], hc.at[b, s], {"gz": zstep, "gy": ystep}))
        ext[R:R + CY, R:R + CZ, :] = value
        return ends

    zi, zj = iota((CZ, CZ + 2 * R), 0), iota((CZ, CZ + 2 * R), 1)
    band_z = band(zj - R - zi)
    xi, xj = iota((CX, CX), 0), iota((CX, CX), 1)
    band_x = band(xi - xj)
    halo_at = jnp.where(xi < R, xi - R, xi - R + CX)
    band_halo = jnp.where(xi < 2 * R, band(halo_at - xj), 0.0)

    def halo_finish(b, ends, between=None):
        for end in ends:
            end()
        f32 = jnp.float32
        for side in (0, 1):
            y0 = 0 if side == 0 else R + CY
            z0 = 0 if side == 0 else R + CZ
            ext[y0:y0 + R, R:R + CZ, :] = hy[b, side].astype(f32)
            ext[R:R + CY, z0:z0 + R, :] = hz[b, side].astype(f32)
            for ys in (0, 1):
                yy = 0 if ys == 0 else R + CY
                ext[yy:yy + R, z0:z0 + R, :] = hc[b, side * 2 + ys].astype(f32)

        def one(y, carry):
            total = TAPS[0] * ext[y]
            for k in range(1, 2 * R + 1):
                total = total + TAPS[k] * ext[y + k]
            yb[y] = total
            return carry
        lax.fori_loop(0, CY, one, 0)
        wide = jnp.concatenate([yb[y] for y in range(CY)], axis=1)
        zb = dot(band_z, wide, HIGH)
        rows = jnp.concatenate([zb[:, y * CX:(y + 1) * CX] for y in range(CY)], axis=0)
        turned = rows.T
        x_send[0] = turned[CX - R:]
        x_send[1] = turned[:R]
        xends = [shift_send(x_send.at[side], x_recv.at[b, side], x_recv.at[b, side], {"gx": step})
                 for side, step in ((0, 1), (1, -1))]
        result = dot(rows, band_x, HIGH)
        if between is not None:
            between()
        for end in xends:
            end()
        edge = jnp.concatenate([x_recv[b, 0], x_recv[b, 1], jnp.zeros((CX - 2 * R, CY * CZ), jnp.float32)], axis=0)
        return result + dot(edge.T, band_halo, HIGH)

    def rims_start(n, value):
        fy_send[0] = value[CY - 1]
        fy_send[1] = value[0]
        fz_send[0] = value[:, CZ - 1, :]
        fz_send[1] = value[:, 0, :]
        turned = value.reshape(CY * CZ, CX).T
        fx_send[0] = turned[CX - 8:]
        fx_send[1] = turned[:8]
        ends = []
        for buf, got, axis in ((fy_send, fy, "gy"), (fz_send, fz, "gz"), (fx_send, fx, "gx")):
            for side, step in ((0, 1), (1, -1)):
                ends.append(shift_send(buf.at[side], got.at[n, side], got.at[n, side], {axis: step}))
        return ends

    shape = (CY, CZ, CX)
    iy, iz, ix = iota(shape, 0), iota(shape, 1), iota(shape, 2)

    def differences(n, value, ends):
        for end in ends:
            end()
        zeros = jnp.zeros((CX - 16, CY * CZ), jnp.float32)
        xcol = jnp.concatenate([fx[n, 0][7:8], jnp.zeros((CX - 2, CY * CZ), jnp.float32), fx[n, 1][0:1]], axis=0).T.reshape(shape)
        del zeros
        uppers = [
            jnp.where(iz == CZ - 1, fz[n, 1][:, None, :], pltpu.roll(value, CZ - 1, 1)),
            jnp.concatenate([value[1:], fy[n, 1][None]], axis=0),
            jnp.where(ix == CX - 1, xcol, pltpu.roll(value, CX - 1, 2)),
        ]
        lowers = [
            jnp.where(iz == 0, fz[n, 0][:, None, :], pltpu.roll(value, 1, 1)),
            jnp.concatenate([fy[n, 0][None], value[:-1]], axis=0),
            jnp.where(ix == 0, xcol, pltpu.roll(value, 1, 2)),
        ]
        jumps, before = [], []
        for axis, where, upper, lower, extent in zip(AXES, (iz, iy, ix), uppers, lowers, (CZ, CY, CX)):
            place = where + at[axis] * extent
            jumps.append(jnp.where(place == extent * sizes[axis] - 1, 0.0, upper - value))
            before.append(jnp.where(place == 0, 0.0, value - lower))
        return jumps, before

    def whole(scalar):
        return jnp.broadcast_to(scalar, (CZ, CX))[None]

    def soft(v, cut):
        return v - jnp.clip(v, -cut, cut)

    def sums_start(n, stage, value):
        slots = sum_send.at[n, stage]
        slots[...] = value
        copies = []
        axes_n = sizes["gz"] if stage == 0 else bricks
        for o in range(1, axes_n):
            if stage == 0:
                target = {"gz": lax.rem(at["gz"] + o, axes_n)}
            else:
                s = lax.rem(me + o, bricks)
                target = {"gy": s // ngx, "gx": lax.rem(s, ngx)}
            copy = remote(slots, sum_recv.at[n, stage, o], target)
            copy.start()
            copies.append(copy)
        return copies

    def sums_finish(n, stage, copies):
        total = sum_send[n, stage]
        for o, copy in enumerate(copies, 1):
            copy.wait()
            total = total + sum_recv[n, stage, o]
        return total

    def exchange(src_of, dst):
        copies = []
        for o in range(1, bricks):
            s = lax.rem(me + o, bricks)
            copy = remote(src_of(s), dst, {"gy": s // ngx, "gx": lax.rem(s, ngx)})
            copy.start()
            copies.append(copy)
        return copies

    value = jnp.swapaxes(start_ref[...], 0, 1)
    field_ref[...] = value
    halo_ends = halo_start(0, value)
    rim_ends = rims_start(0, value)
    relayout()
    value = field_ref[...]
    jumps, before = differences(0, value, rim_ends)
    penalty = jnp.full((1, 1), rho_start, jnp.float32)
    cutoff = shrink_weight / penalty
    smoothing, back = None, None
    for d in range(3):
        term = before[d] - jumps[d]
        cut = whole(cutoff)
        shr = soft(before[d], cut) - soft(jumps[d], cut)
        smoothing = term if smoothing is None else smoothing + term
        back = shr if back is None else back + shr
    base_ref[0] = smoothing
    base_ref[1] = jnp.zeros_like(smoothing)
    back_ref[...] = back
    sub = iota((ANG, DW), 0)
    tables = []

    for sweep in range(ITERS):
        last = sweep + 1 == ITERS
        pending = {}

        def between():
            if sweep:
                total = sums_finish(sweep - 1, 0, pending0["copies"])
                pending["copies"] = sums_start(sweep - 1, 1, total)
        pending0 = {"copies": sums_copies} if sweep else {}
        blurred = halo_finish(2 * sweep, halo_ends, between)
        flat[...] = jnp.concatenate([blurred[y * CZ:(y + 1) * CZ] for y in range(CY)], axis=1).astype(jnp.bfloat16)

        def forward(a, carry):
            proj[pl.ds(pl.multiple_of(a * CZ, CZ), CZ), :] = dot(flat[...], mats[a]).astype(jnp.bfloat16)
            return carry
        lax.fori_loop(0, ANG, forward, 0)
        send1[sweep] = permute(proj[...], True).reshape(CZ, ANG, DW).astype(jnp.bfloat16)
        copies = exchange(lambda s: send1.at[sweep, pl.ds(s * owned, owned)], recv1.at[sweep, me])
        recv1[sweep, me] = send1[sweep, pl.ds(me * owned, owned)]
        which = jnp.zeros((ANG, DET_OF(measured_ref)), jnp.int32)
        lane = iota(which.shape, 0)
        for a in range(ANG):
            which = jnp.where(lane == a, rows_ref[a], which)
        observed = jnp.zeros(measured_ref.shape, jnp.float32)
        for k in range(ANG):
            observed = jnp.where((which == k)[None], measured_ref[:, k:k + 1, :], observed)
        if sweep == 0:
            for s in range(bricks):
                t = jnp.zeros((ANG, DW), jnp.int32)
                for a in range(ANG):
                    t = jnp.where(sub == a, table_ref[s * ANG + a], t)
                tables.append(t)
        else:
            total = sums_finish(sweep - 1, 1, pending["copies"])
            primal_res = jnp.sum(total[0:1], axis=1, keepdims=True) / (3.0 * cells)
            dual_res = penalty * penalty * jnp.sum(total[1:2], axis=1, keepdims=True) / cells
            factor = jnp.sqrt(jnp.sqrt((primal_res + eps_norm) / (dual_res + eps_norm)))
            penalty = penalty * factor
            cutoff = shrink_weight / penalty
            for d in range(3):
                dual_s[d] = dual_s[d] / whole(factor)
                dlow_s[d] = dlow_s[d] / whole(factor)
            base_ref[1] = base_ref[1] / whole(factor)
        for copy in copies:
            copy.wait()
        sino = [jnp.zeros((owned, ANG, DW), jnp.float32) for _ in range(NBLK)]
        for s in range(bricks):
            got = recv1[sweep, s].astype(jnp.float32)
            for q in range(NBLK):
                sino[q] = sino[q] + jnp.where((tables[s] == q)[None], got, 0.0)
        for q in range(NBLK):
            sino[q] = sino[q] - observed[:, :, q * DW:(q + 1) * DW]
        for s in range(bricks):
            chosen = sino[0]
            for q in range(1, NBLK):
                chosen = jnp.where((tables[s] == q)[None], sino[q], chosen)
            send2[sweep, s] = chosen.astype(jnp.bfloat16)
        place = pl.ds(me * owned, owned)
        copies = exchange(lambda s: send2.at[sweep, s], arrived.at[sweep, place])
        arrived[sweep, place] = send2[sweep, me]
        for copy in copies:
            copy.wait()
        got = arrived[sweep].astype(jnp.float32).reshape(CZ * ANG, DW).astype(jnp.bfloat16)
        misfit[...] = permute(got, False).astype(jnp.bfloat16)

        part = V // 8

        def backward(n, carry):
            total = jnp.zeros((CZ, part), jnp.float32)
            for a in range(ANG):
                total = total + lax.dot_general(
                    misfit[a * CZ:(a + 1) * CZ, :], mats[a, pl.ds(pl.multiple_of(n * part, part), part), :],
                    (((1,), (1,)), ((), ())), preferred_element_type=jnp.float32)
            per_part = part // CX
            for i in range(per_part):
                estimate_rows[n * per_part + i] = total[:, i * CX:(i + 1) * CX]
            return carry
        estimate_rows = yb_rows(yb, CZ)
        lax.fori_loop(0, 8, backward, 0)
        halo_ends = halo_start(2 * sweep + 1, estimate_rows[...])
        grad = halo_finish(2 * sweep + 1, halo_ends).reshape(shape)
        value = field_ref[...] - step_size * (
            grad + whole(penalty) * (base_ref[0] + base_ref[1] - back_ref[...]))
        field_ref[...] = value
        rim_ends = rims_start(sweep + 1, value)
        if not last:
            halo_ends = halo_start(2 * sweep + 2, value)
        else:
            estimate_ref[...] = jnp.swapaxes(value, 0, 1)
        jumps, before = differences(sweep + 1, value, rim_ends)
        cut = whole(cutoff)
        primal = jnp.zeros((CZ, CX), jnp.float32)
        smoothing, back_new, back_dual = [jnp.zeros(shape, jnp.float32)] * 3
        for d in range(3):
            smoothing = smoothing + (before[d] - jumps[d])
            if sweep:
                total, low = jumps[d] + dual_s[d], before[d] + dlow_s[d]
            else:
                total, low = jumps[d], before[d]
            shr, shr_low = soft(total, cut), soft(low, cut)
            new, new_low = total - shr, low - shr_low
            dual_s[d] = new
            if not last:
                dlow_s[d] = new_low
                back_dual = back_dual + (new_low - new)
            back_new = back_new + (shr_low - shr)
            gap = jumps[d] - shr
            primal = primal + jnp.sum(gap * gap, axis=0)
        change = back_new - back_ref[...]
        dual_part = jnp.sum(change * change, axis=0)
        sums = jnp.concatenate([
            jnp.sum(primal, axis=0, keepdims=True), jnp.sum(dual_part, axis=0, keepdims=True),
            jnp.zeros((6, CX), jnp.float32)], axis=0)
        if not last:
            base_ref[0] = smoothing
            base_ref[1] = back_dual
            back_ref[...] = back_new
        sums_copies = sums_start(sweep, 0, sums)

    total = sums_finish(ITERS - 1, 0, sums_copies)
    final_copies = sums_start(ITERS - 1, 1, total)
    for d in range(3):
        dual_ref[d] = jnp.swapaxes(dual_s[d], 0, 1)
    total = sums_finish(ITERS - 1, 1, final_copies)
    primal_res = jnp.sum(total[0:1], axis=1, keepdims=True) / (3.0 * cells)
    dual_res = penalty * penalty * jnp.sum(total[1:2], axis=1, keepdims=True) / cells
    factor = jnp.sqrt(jnp.sqrt((primal_res + eps_norm) / (dual_res + eps_norm)))
    final = jnp.broadcast_to(factor, (CY, CX))[None]
    for d in range(3):
        dual_ref[d] = dual_ref[d] / final


def DET_OF(ref):
    return ref.shape[2]


def yb_rows(ref, depth):
    return ref.at[:, pl.ds(0, depth), :]


def body(sizes, start, measured, tiles, tile_block, angle_row):
    CZ, CY, CX = start.shape
    V, ANG, DW = tiles.shape
    owned = measured.shape[0]
    bricks = sizes["gy"] * sizes["gx"]
    R = RADIUS
    f32, bf16 = jnp.float32, jnp.bfloat16
    blurs, rims = 2 * ITERS, ITERS + 1
    slots = blurs * 10 + rims * 6 + ITERS * (2 * (bricks - 1) + bricks - 1 + sizes["gz"] - 1)
    vm = pltpu.VMEM
    scratch = [
        vm((V * ANG, DW), bf16), vm((ANG, V, DW), bf16), vm((CY + 2 * R, CZ + 2 * R, CX), f32),
        vm((CY, CZ + 2 * R, CX), f32), vm((CZ, V), bf16), vm((ANG * CZ, DW), bf16),
        vm((ITERS, CZ, ANG, DW), bf16), vm((ITERS, bricks, owned, ANG, DW), bf16),
        vm((ITERS, bricks, owned, ANG, DW), bf16), vm((ITERS, CZ, ANG, DW), bf16), vm((ANG * CZ, DW), bf16),
        vm((2, R, CZ, CX), bf16), vm((2, CY, R, CX), bf16), vm((4, R, R, CX), bf16),
        vm((blurs, 2, R, CZ, CX), bf16), vm((blurs, 2, CY, R, CX), bf16), vm((blurs, 4, R, R, CX), bf16),
        vm((2, R, CY * CZ), f32), vm((blurs, 2, R, CY * CZ), f32),
        vm((2, CZ, CX), f32), vm((2, CY, CX), f32), vm((2, 8, CY * CZ), f32),
        vm((rims, 2, CZ, CX), f32), vm((rims, 2, CY, CX), f32), vm((rims, 2, 8, CY * CZ), f32),
        vm((ITERS, 2, 8, CX), f32), vm((ITERS, 2, max(bricks, sizes["gz"]), 8, CX), f32),
        vm((CY, CZ, CX), f32), vm((2, CY, CZ, CX), f32), vm((CY, CZ, CX), f32),
        vm((3, CY, CZ, CX), f32), vm((3, CY, CZ, CX), f32),
        pltpu.SemaphoreType.DMA((slots,)), pltpu.SemaphoreType.DMA((slots,)), pltpu.SemaphoreType.DMA((8,)),
    ]
    vmem = pl.BlockSpec(memory_space=pltpu.VMEM)
    smem = pl.BlockSpec(memory_space=pltpu.SMEM)
    return pl.pallas_call(
        functools.partial(kernel, sizes, (CZ, CY, CX, ANG, DW, V, owned)),
        out_shape=(jax.ShapeDtypeStruct((CZ, CY, CX), f32), jax.ShapeDtypeStruct((3, CZ, CY, CX), f32)),
        in_specs=[vmem, vmem, pl.BlockSpec(memory_space=pl.ANY), smem, smem],
        out_specs=(vmem, vmem),
        scratch_shapes=scratch,
        compiler_params=pltpu.CompilerParams(has_side_effects=True, vmem_limit_bytes=60 * 1024 * 1024),
    )(start, measured, tiles.reshape(V * ANG, DW), tile_block.reshape(-1), angle_row)


def solution(mesh):
    return jax.shard_map(
        functools.partial(body, dict(mesh.shape)),
        mesh=mesh,
        in_specs=(
            P("gz", "gy", "gx"),
            P(("gz", "gy", "gx"), None, None),
            P("gy", None, "gx"),
            P(),
            P(),
        ),
        out_specs=(P("gz", "gy", "gx"), P(None, "gz", "gy", "gx")),
        check_vma=False,
    )
```

```python
import functools
import math

import jax
import jax.numpy as jnp
from jax import lax
from jax.experimental import pallas as pl
from jax.experimental.pallas import tpu as pltpu
from jax.sharding import PartitionSpec as P

RADIUS = 8
ITERS = 2
NBLK = 4

blur_sigma = 2.5
step_size = 0.5
shrink_weight = 0.2
rho_start = 1.0
eps_norm = 1e-06

AXES = ("gz", "gy", "gx")
MESH = pl.DeviceIdType.MESH
HIGH = lax.Precision.HIGHEST
SPREAD = 2.0 * blur_sigma * blur_sigma
NORM = 1.0 / sum(math.exp(-k * k / SPREAD) for k in range(-RADIUS, RADIUS + 1))
TAPS = [NORM * math.exp(-k * k / SPREAD) for k in range(-RADIUS, RADIUS + 1)]
FACES = [(axis, side) for axis in AXES for side in (-1, 1)]
HALOS = [(dz, dy) for dz in (-1, 0, 1) for dy in (-1, 0, 1) if dz or dy]


def band(distance):
    near = jnp.abs(distance) <= RADIUS
    d = distance.astype(jnp.float32)
    return jnp.where(near, jnp.exp(-d * d / SPREAD) * NORM, 0.0)


def iota(shape, dim):
    return lax.broadcasted_iota(jnp.int32, shape, dim)


def dot(a, b, precision=None):
    return jnp.dot(a, b, preferred_element_type=jnp.float32, precision=precision)


def kernel(sizes, dims, start_hbm, measured_hbm, tiles_ref, table_hbm, rows_hbm, estimate_hbm, dual_hbm, factor_ref, *scratch):
    (raw, mats, ext, yb, flat, proj, send1, recv1, send2, arrived, misfit,
     hy_send, hz_send, hc_send, hy, hz, hc, x_send, x_recv, fy_send, fz_send, fx_send, fy, fz, fx,
     sum_send, sum_recv, field_ref, base_ref, back_ref, dual_s, dlow_s, start_ref, measured_ref, estimate_ref, dual_ref, table_ref, rows_ref, send_sem, recv_sem, load_sem, io_sem) = scratch
    CZ, CY, CX, ANG, DW, V, owned = dims
    bricks = sizes["gy"] * sizes["gx"]
    ngx = sizes["gx"]
    at = {axis: lax.axis_index(axis) for axis in AXES}
    me = at["gy"] * ngx + at["gx"]
    counter = [0]
    R = RADIUS
    cells = float(CZ * CY * CX * sizes["gz"] * bricks)

    def exists(steps):
        ok = None
        for axis, step in steps.items():
            if step == 0:
                continue
            test = at[axis] > 0 if step < 0 else at[axis] < sizes[axis] - 1
            ok = test if ok is None else jnp.logical_and(ok, test)
        return ok

    def remote(src, dst, target):
        slot = counter[0]
        counter[0] += 1
        return pltpu.make_async_remote_copy(
            src_ref=src, dst_ref=dst, send_sem=send_sem.at[slot], recv_sem=recv_sem.at[slot],
            device_id=target, device_id_type=MESH)

    def shift_send(src, dst_here, dst_there, steps):
        target = {axis: lax.rem(at[axis] + step + sizes[axis], sizes[axis]) for axis, step in steps.items() if step}
        copy = remote(src, dst_there, target)
        out_ok = exists(steps)
        in_ok = exists({axis: -step for axis, step in steps.items()})

        @pl.when(out_ok)
        def _():
            copy.start()

        @pl.when(jnp.logical_not(in_ok))
        def _():
            dst_here[...] = jnp.zeros(dst_here.shape, dst_here.dtype)

        def finish():
            @pl.when(out_ok)
            def _():
                copy.wait_send()

            @pl.when(in_ok)
            def _():
                copy.wait_recv()
        return finish

    chunks = 8
    per = V * ANG // chunks
    loads = [pltpu.make_async_copy(tiles_ref.at[pl.ds(i * per, per)], raw.at[pl.ds(i * per, per)], load_sem.at[i])
             for i in range(chunks)]
    start_load = pltpu.make_async_copy(start_hbm, start_ref, io_sem.at[0])
    measured_load = pltpu.make_async_copy(measured_hbm, measured_ref, io_sem.at[1])
    start_load.start()

    barrier = pltpu.get_barrier_semaphore()
    partners = 0
    for o in range(1, bricks):
        s = lax.rem(me + o, bricks)
        pl.semaphore_signal(barrier, inc=1, device_id={"gy": s // ngx, "gx": lax.rem(s, ngx)}, device_id_type=MESH)
        partners += 1
    for o in range(1, sizes["gz"]):
        pl.semaphore_signal(barrier, inc=1, device_id={"gz": lax.rem(at["gz"] + o, sizes["gz"])}, device_id_type=MESH)
        partners += 1
    corners = [{"gz": dz, "gy": dy} for dz in (-1, 1) for dy in (-1, 1)]
    for steps in corners:
        target = {axis: lax.rem(at[axis] + step + sizes[axis], sizes[axis]) for axis, step in steps.items()}
        pl.semaphore_signal(barrier, inc=1, device_id=target, device_id_type=MESH)
        partners += 1
    for load in loads:
        load.start()
    small_loads = [measured_load, pltpu.make_async_copy(table_hbm, table_ref, io_sem.at[4]),
                   pltpu.make_async_copy(rows_hbm, rows_ref, io_sem.at[5])]
    for load in small_loads:
        load.start()
    group = 256 // ANG
    r, c = iota((256, 256), 0), iota((256, 256), 1)
    to_major = jnp.where((r // group == c % ANG) & (r % group == c // ANG), 1.0, 0.0).astype(jnp.bfloat16)

    def relayout():
        steps = per // 256
        for i in range(chunks):
            loads[i].wait()

            def one(n, carry):
                block = raw[pl.ds(pl.multiple_of(i * per + n * 256, 256), 256), :]
                moved = dot(to_major, block).astype(jnp.bfloat16)
                first = pl.multiple_of((i * steps + n) * group, group)
                for a in range(ANG):
                    mats[a, pl.ds(first, group), :] = moved[a * group:(a + 1) * group]
                return carry
            lax.fori_loop(0, steps, one, 0, unroll=True)

    def permute(block, transposed):
        n = CZ * ANG
        rr, cc = iota((n, n), 0), iota((n, n), 1)
        if transposed:
            m = (rr // ANG == cc % CZ) & (rr % ANG == cc // CZ)
        else:
            m = (rr // CZ == cc % ANG) & (rr % CZ == cc // ANG)
        return dot(jnp.where(m, 1.0, 0.0).astype(jnp.bfloat16), block)

    def halo_start(b, value):
        low = value.astype(jnp.bfloat16)
        hy_send[0] = low[CY - R:]
        hy_send[1] = low[:R]
        zl, zh = value[:, CZ - R:, :].astype(jnp.bfloat16), value[:, :R, :].astype(jnp.bfloat16)
        hz_send[0] = zl
        hz_send[1] = zh
        hc_send[0] = zl[CY - R:]
        hc_send[1] = zl[:R]
        hc_send[2] = zh[CY - R:]
        hc_send[3] = zh[:R]
        ends = []
        for side, step in ((0, 1), (1, -1)):
            ends.append(shift_send(hy_send.at[side], hy.at[b, side], hy.at[b, side], {"gy": step}))
            ends.append(shift_send(hz_send.at[side], hz.at[b, side], hz.at[b, side], {"gz": step}))
        for zs, zstep in ((0, 1), (1, -1)):
            for ys, ystep in ((0, 1), (1, -1)):
                s = zs * 2 + ys
                ends.append(shift_send(hc_send.at[s], hc.at[b, s], hc.at[b, s], {"gz": zstep, "gy": ystep}))
        ext[R:R + CY, R:R + CZ, :] = value
        return ends

    zi, zj = iota((CZ, CZ + 2 * R), 0), iota((CZ, CZ + 2 * R), 1)
    band_z = band(zj - R - zi)
    xi, xj = iota((CX, CX), 0), iota((CX, CX), 1)
    band_x = band(xi - xj)
    halo_at = jnp.where(xi < R, xi - R, xi - R + CX)
    band_halo = jnp.where(xi < 2 * R, band(halo_at - xj), 0.0)

    def halo_finish(b, ends, between=None):
        for end in ends:
            end()
        f32 = jnp.float32
        for side in (0, 1):
            y0 = 0 if side == 0 else R + CY
            z0 = 0 if side == 0 else R + CZ
            ext[y0:y0 + R, R:R + CZ, :] = hy[b, side].astype(f32)
            ext[R:R + CY, z0:z0 + R, :] = hz[b, side].astype(f32)
            for ys in (0, 1):
                yy = 0 if ys == 0 else R + CY
                ext[yy:yy + R, z0:z0 + R, :] = hc[b, side * 2 + ys].astype(f32)

        def one(y, carry):
            total = TAPS[0] * ext[y]
            for k in range(1, 2 * R + 1):
                total = total + TAPS[k] * ext[y + k]
            yb[y] = total
            return carry
        lax.fori_loop(0, CY, one, 0)
        wide = jnp.concatenate([yb[y] for y in range(CY)], axis=1)
        zb = dot(band_z, wide, HIGH)
        rows = jnp.concatenate([zb[:, y * CX:(y + 1) * CX] for y in range(CY)], axis=0)
        turned = rows.T
        x_send[0] = turned[CX - R:]
        x_send[1] = turned[:R]
        xends = [shift_send(x_send.at[side], x_recv.at[b, side], x_recv.at[b, side], {"gx": step})
                 for side, step in ((0, 1), (1, -1))]
        result = dot(rows, band_x, HIGH)
        if between is not None:
            between()
        for end in xends:
            end()
        edge = jnp.concatenate([x_recv[b, 0], x_recv[b, 1], jnp.zeros((CX - 2 * R, CY * CZ), jnp.float32)], axis=0)
        return result + dot(edge.T, band_halo, HIGH)

    def rims_start(n, value):
        fy_send[0] = value[CY - 1]
        fy_send[1] = value[0]
        fz_send[0] = value[:, CZ - 1, :]
        fz_send[1] = value[:, 0, :]
        turned = value.reshape(CY * CZ, CX).T
        fx_send[0] = turned[CX - 8:]
        fx_send[1] = turned[:8]
        ends = []
        for buf, got, axis in ((fy_send, fy, "gy"), (fz_send, fz, "gz"), (fx_send, fx, "gx")):
            for side, step in ((0, 1), (1, -1)):
                ends.append(shift_send(buf.at[side], got.at[n, side], got.at[n, side], {axis: step}))
        return ends

    shape = (CY, CZ, CX)
    iy, iz, ix = iota(shape, 0), iota(shape, 1), iota(shape, 2)

    def differences(n, value, ends):
        for end in ends:
            end()
        zeros = jnp.zeros((CX - 16, CY * CZ), jnp.float32)
        xcol = jnp.concatenate([fx[n, 0][7:8], jnp.zeros((CX - 2, CY * CZ), jnp.float32), fx[n, 1][0:1]], axis=0).T.reshape(shape)
        del zeros
        uppers = [
            jnp.where(iz == CZ - 1, fz[n, 1][:, None, :], pltpu.roll(value, CZ - 1, 1)),
            jnp.concatenate([value[1:], fy[n, 1][None]], axis=0),
            jnp.where(ix == CX - 1, xcol, pltpu.roll(value, CX - 1, 2)),
        ]
        lowers = [
            jnp.where(iz == 0, fz[n, 0][:, None, :], pltpu.roll(value, 1, 1)),
            jnp.concatenate([fy[n, 0][None], value[:-1]], axis=0),
            jnp.where(ix == 0, xcol, pltpu.roll(value, 1, 2)),
        ]
        jumps, before = [], []
        for axis, where, upper, lower, extent in zip(AXES, (iz, iy, ix), uppers, lowers, (CZ, CY, CX)):
            place = where + at[axis] * extent
            jumps.append(jnp.where(place == extent * sizes[axis] - 1, 0.0, upper - value))
            before.append(jnp.where(place == 0, 0.0, value - lower))
        return jumps, before

    def whole(scalar):
        return jnp.broadcast_to(scalar, (CZ, CX))[None]

    def soft(v, cut):
        return v - jnp.clip(v, -cut, cut)

    def sums_start(n, stage, value):
        slots = sum_send.at[n, stage]
        slots[...] = value
        copies = []
        axes_n = sizes["gz"] if stage == 0 else bricks
        for o in range(1, axes_n):
            if stage == 0:
                target = {"gz": lax.rem(at["gz"] + o, axes_n)}
            else:
                s = lax.rem(me + o, bricks)
                target = {"gy": s // ngx, "gx": lax.rem(s, ngx)}
            copy = remote(slots, sum_recv.at[n, stage, o], target)
            copy.start()
            copies.append(copy)
        return copies

    def sums_finish(n, stage, copies):
        total = sum_send[n, stage]
        for o, copy in enumerate(copies, 1):
            copy.wait()
            total = total + sum_recv[n, stage, o]
        return total

    def exchange(src_of, dst):
        copies = []
        for o in range(1, bricks):
            s = lax.rem(me + o, bricks)
            copy = remote(src_of(s), dst, {"gy": s // ngx, "gx": lax.rem(s, ngx)})
            copy.start()
            copies.append(copy)
        return copies

    start_load.wait()
    value = jnp.swapaxes(start_ref[...], 0, 1)
    field_ref[...] = value
    pl.semaphore_wait(barrier, partners)
    halo_ends = halo_start(0, value)
    rim_ends = rims_start(0, value)
    relayout()
    for load in small_loads:
        load.wait()
    value = field_ref[...]
    jumps, before = differences(0, value, rim_ends)
    penalty = jnp.full((1, 1), rho_start, jnp.float32)
    cutoff = shrink_weight / penalty
    smoothing, back = None, None
    for d in range(3):
        term = before[d] - jumps[d]
        cut = whole(cutoff)
        shr = soft(before[d], cut) - soft(jumps[d], cut)
        smoothing = term if smoothing is None else smoothing + term
        back = shr if back is None else back + shr
    base_ref[0] = smoothing
    base_ref[1] = jnp.zeros_like(smoothing)
    back_ref[...] = back
    sub = iota((ANG, DW), 0)
    tables = []

    for sweep in range(ITERS):
        last = sweep + 1 == ITERS
        pending = {}

        def between():
            if sweep:
                total = sums_finish(sweep - 1, 0, pending0["copies"])
                pending["copies"] = sums_start(sweep - 1, 1, total)
        pending0 = {"copies": sums_copies} if sweep else {}
        blurred = halo_finish(2 * sweep, halo_ends, between)
        flat[...] = jnp.concatenate([blurred[y * CZ:(y + 1) * CZ] for y in range(CY)], axis=1).astype(jnp.bfloat16)

        def forward(a, carry):
            proj[pl.ds(pl.multiple_of(a * CZ, CZ), CZ), :] = dot(flat[...], mats[a]).astype(jnp.bfloat16)
            return carry
        lax.fori_loop(0, ANG, forward, 0, unroll=4)
        send1[sweep] = permute(proj[...], True).reshape(CZ, ANG, DW).astype(jnp.bfloat16)
        copies = exchange(lambda s: send1.at[sweep, pl.ds(s * owned, owned)], recv1.at[sweep, me])
        recv1[sweep, me] = send1[sweep, pl.ds(me * owned, owned)]
        which = jnp.zeros((ANG, DET_OF(measured_ref)), jnp.int32)
        lane = iota(which.shape, 0)
        for a in range(ANG):
            which = jnp.where(lane == a, rows_ref[a], which)
        observed = jnp.zeros(measured_ref.shape, jnp.float32)
        for k in range(ANG):
            observed = jnp.where((which == k)[None], measured_ref[:, k:k + 1, :], observed)
        if sweep == 0:
            for s in range(bricks):
                t = jnp.zeros((ANG, DW), jnp.int32)
                for a in range(ANG):
                    t = jnp.where(sub == a, table_ref[s // ngx, s % ngx, a], t)
                tables.append(t)
        else:
            total = sums_finish(sweep - 1, 1, pending["copies"])
            primal_res = jnp.sum(total[0:1], axis=1, keepdims=True) / (3.0 * cells)
            dual_res = penalty * penalty * jnp.sum(total[1:2], axis=1, keepdims=True) / cells
            factor = jnp.sqrt(jnp.sqrt((primal_res + eps_norm) / (dual_res + eps_norm)))
            penalty = penalty * factor
            cutoff = shrink_weight / penalty
            for d in range(3):
                dual_s[d] = dual_s[d] / whole(factor)
                dlow_s[d] = dlow_s[d] / whole(factor)
            base_ref[1] = base_ref[1] / whole(factor)
        for copy in copies:
            copy.wait()
        sino = [jnp.zeros((owned, ANG, DW), jnp.float32) for _ in range(NBLK)]
        for s in range(bricks):
            got = recv1[sweep, s].astype(jnp.float32)
            for q in range(NBLK):
                sino[q] = sino[q] + jnp.where((tables[s] == q)[None], got, 0.0)
        for q in range(NBLK):
            sino[q] = sino[q] - observed[:, :, q * DW:(q + 1) * DW]
        for s in range(bricks):
            chosen = sino[0]
            for q in range(1, NBLK):
                chosen = jnp.where((tables[s] == q)[None], sino[q], chosen)
            send2[sweep, s] = chosen.astype(jnp.bfloat16)
        place = pl.ds(me * owned, owned)
        copies = exchange(lambda s: send2.at[sweep, s], arrived.at[sweep, place])
        arrived[sweep, place] = send2[sweep, me]
        for copy in copies:
            copy.wait()
        got = arrived[sweep].astype(jnp.float32).reshape(CZ * ANG, DW).astype(jnp.bfloat16)
        misfit[...] = permute(got, False).astype(jnp.bfloat16)

        part = V // 8

        def backward(n, carry):
            total = jnp.zeros((CZ, part), jnp.float32)
            for a in range(ANG):
                total = total + lax.dot_general(
                    misfit[a * CZ:(a + 1) * CZ, :], mats[a, pl.ds(pl.multiple_of(n * part, part), part), :],
                    (((1,), (1,)), ((), ())), preferred_element_type=jnp.float32)
            per_part = part // CX
            for i in range(per_part):
                estimate_rows[n * per_part + i] = total[:, i * CX:(i + 1) * CX]
            return carry
        estimate_rows = yb_rows(yb, CZ)
        lax.fori_loop(0, 8, backward, 0, unroll=4)
        halo_ends = halo_start(2 * sweep + 1, estimate_rows[...])
        grad = halo_finish(2 * sweep + 1, halo_ends).reshape(shape)
        value = field_ref[...] - step_size * (
            grad + whole(penalty) * (base_ref[0] + base_ref[1] - back_ref[...]))
        field_ref[...] = value
        rim_ends = rims_start(sweep + 1, value)
        if not last:
            halo_ends = halo_start(2 * sweep + 2, value)
        else:
            estimate_ref[...] = jnp.swapaxes(value, 0, 1)
            estimate_out = pltpu.make_async_copy(estimate_ref, estimate_hbm, io_sem.at[2])
            estimate_out.start()
        jumps, before = differences(sweep + 1, value, rim_ends)
        cut = whole(cutoff)
        primal = jnp.zeros((CZ, CX), jnp.float32)
        smoothing, back_new, back_dual = [jnp.zeros(shape, jnp.float32)] * 3
        for d in range(3):
            smoothing = smoothing + (before[d] - jumps[d])
            if sweep:
                total, low = jumps[d] + dual_s[d], before[d] + dlow_s[d]
            else:
                total, low = jumps[d], before[d]
            shr, shr_low = soft(total, cut), soft(low, cut)
            new, new_low = total - shr, low - shr_low
            dual_s[d] = new
            if not last:
                dlow_s[d] = new_low
                back_dual = back_dual + (new_low - new)
            back_new = back_new + (shr_low - shr)
            gap = jumps[d] - shr
            primal = primal + jnp.sum(gap * gap, axis=0)
        change = back_new - back_ref[...]
        dual_part = jnp.sum(change * change, axis=0)
        sums = jnp.concatenate([
            jnp.sum(primal, axis=0, keepdims=True), jnp.sum(dual_part, axis=0, keepdims=True)], axis=0)
        if not last:
            base_ref[0] = smoothing
            base_ref[1] = back_dual
            back_ref[...] = back_new
        sums_copies = sums_start(sweep, 0, sums)

    total = sums_finish(ITERS - 1, 0, sums_copies)
    final_copies = sums_start(ITERS - 1, 1, total)
    for d in range(3):
        dual_ref[d] = jnp.swapaxes(dual_s[d], 0, 1)
    dual_out = pltpu.make_async_copy(dual_ref, dual_hbm, io_sem.at[3])
    dual_out.start()
    total = sums_finish(ITERS - 1, 1, final_copies)
    primal_res = jnp.sum(total[0:1], axis=1, keepdims=True) / (3.0 * cells)
    dual_res = penalty * penalty * jnp.sum(total[1:2], axis=1, keepdims=True) / cells
    factor = jnp.sqrt(jnp.sqrt((primal_res + eps_norm) / (dual_res + eps_norm)))
    factor_ref[...] = jnp.broadcast_to(factor, factor_ref.shape)
    estimate_out.wait()
    dual_out.wait()


def finish(estimate_ref, dual_ref, factor_ref, estimate_out, dual_out):
    estimate_out[...] = estimate_ref[...]
    factor = jnp.broadcast_to(factor_ref[0:1, :], estimate_ref.shape[1:])[None]
    for d in range(3):
        dual_out[d] = dual_ref[d] / factor


def DET_OF(ref):
    return ref.shape[2]


def yb_rows(ref, depth):
    return ref.at[:, pl.ds(0, depth), :]


def body(sizes, start, measured, tiles, tile_block, angle_row):
    CZ, CY, CX = start.shape
    V, ANG, DW = tiles.shape
    owned = measured.shape[0]
    bricks = sizes["gy"] * sizes["gx"]
    R = RADIUS
    f32, bf16 = jnp.float32, jnp.bfloat16
    blurs, rims = 2 * ITERS, ITERS + 1
    slots = blurs * 10 + rims * 6 + ITERS * (2 * (bricks - 1) + bricks - 1 + sizes["gz"] - 1)
    vm = pltpu.VMEM
    scratch = [
        vm((V * ANG, DW), bf16), vm((ANG, V, DW), bf16), vm((CY + 2 * R, CZ + 2 * R, CX), f32),
        vm((CY, CZ + 2 * R, CX), f32), vm((CZ, V), bf16), vm((ANG * CZ, DW), bf16),
        vm((ITERS, CZ, ANG, DW), bf16), vm((ITERS, bricks, owned, ANG, DW), bf16),
        vm((ITERS, bricks, owned, ANG, DW), bf16), vm((ITERS, CZ, ANG, DW), bf16), vm((ANG * CZ, DW), bf16),
        vm((2, R, CZ, CX), bf16), vm((2, CY, R, CX), bf16), vm((4, R, R, CX), bf16),
        vm((blurs, 2, R, CZ, CX), bf16), vm((blurs, 2, CY, R, CX), bf16), vm((blurs, 4, R, R, CX), bf16),
        vm((2, R, CY * CZ), f32), vm((blurs, 2, R, CY * CZ), f32),
        vm((2, CZ, CX), f32), vm((2, CY, CX), f32), vm((2, 8, CY * CZ), f32),
        vm((rims, 2, CZ, CX), f32), vm((rims, 2, CY, CX), f32), vm((rims, 2, 8, CY * CZ), f32),
        vm((ITERS, 2, 2, CX), f32), vm((ITERS, 2, max(bricks, sizes["gz"]), 2, CX), f32),
        vm((CY, CZ, CX), f32), vm((2, CY, CZ, CX), f32), vm((CY, CZ, CX), f32),
        vm((3, CY, CZ, CX), f32), vm((3, CY, CZ, CX), f32),
        vm(start.shape, f32), vm(measured.shape, f32), vm(start.shape, f32), vm((3,) + start.shape, f32),
        pltpu.SMEM(tile_block.shape, jnp.int32), pltpu.SMEM(angle_row.shape, jnp.int32),
        pltpu.SemaphoreType.DMA((slots,)), pltpu.SemaphoreType.DMA((slots,)), pltpu.SemaphoreType.DMA((8,)),
        pltpu.SemaphoreType.DMA((6,)),
    ]
    vmem = pl.BlockSpec(memory_space=pltpu.VMEM)
    hbm = pl.BlockSpec(memory_space=pl.ANY)
    shapes = (jax.ShapeDtypeStruct((CZ, CY, CX), f32), jax.ShapeDtypeStruct((3, CZ, CY, CX), f32))
    estimate, dual, factor = pl.pallas_call(
        functools.partial(kernel, sizes, (CZ, CY, CX, ANG, DW, V, owned)),
        out_shape=shapes + (jax.ShapeDtypeStruct((8, CX), f32),),
        in_specs=[pl.BlockSpec(memory_space=pltpu.HBM)] * 5,
        out_specs=(hbm, hbm, vmem),
        scratch_shapes=scratch,
        compiler_params=pltpu.CompilerParams(
            collective_id=0, has_side_effects=True, vmem_limit_bytes=65900000),
    )(start, measured, tiles.reshape(V * ANG, DW), tile_block, angle_row)
    return pl.pallas_call(
        finish,
        out_shape=shapes,
        in_specs=[vmem, vmem, vmem],
        out_specs=(vmem, vmem),
        compiler_params=pltpu.CompilerParams(vmem_limit_bytes=65900000),
    )(estimate, dual, factor)


def solution(mesh):
    return jax.shard_map(
        functools.partial(body, dict(mesh.shape)),
        mesh=mesh,
        in_specs=(
            P("gz", "gy", "gx"),
            P(("gz", "gy", "gx"), None, None),
            P("gy", None, "gx"),
            P(),
            P(),
        ),
        out_specs=(P("gz", "gy", "gx"), P(None, "gz", "gy", "gx")),
        check_vma=False,
    )
```
